32 devices in a mesh: dp: 1 (over z), ep: 32 (over y, x, core).
Axes of the slice: x: 4, y: 4, z: 1, core: 2. Of those that a mesh axis runs over, the one named last changes fastest.
The devices are a block of a 4x4x8 slice.
Arguments:
- hidden_in: bfloat16 [3072, 2048], P(('dp', 'ep'))
- norm_gain: float32 [2048], replicated
- router_w: float32 [64, 2048], replicated
- w_gate: bfloat16 [64, 2048, 1408], P('ep')
- w_up: bfloat16 [64, 2048, 1408], P('ep')
- w_down: bfloat16 [64, 1408, 2048], P('ep')
- ws_gate: bfloat16 [2048, 2816], replicated
- ws_up: bfloat16 [2048, 2816], replicated
- ws_down: bfloat16 [2816, 2048], replicated
- expert_ids: int32 [3072, 6], P(('dp', 'ep'))
Outputs:
- output: bfloat16 [3072, 2048], P(('dp', 'ep'))
All inputs are finite; a program needn't handle non-finite values.
Results may differ from the reference program's by a relative error of at most 0.00429402.
Values are sent between devices in bfloat16 or wider.
A program may use at most 768 MiB of HBM per device.

```python
import jax
import jax.numpy as jnp
from jax import lax

TOKENS = 3072
D = 2048
EXPERTS = 64
INTER = 1408
SHARED_INTER = 2816
TOP = 6
GROUPS = 8
GROUP_LIMIT = 4

NORM_EPS = 1e-6
ROUTE_SCALE = 2.5
GROUP_WIDTH = EXPERTS // GROUPS
SLOT_PAIRS = (TOP + GROUP_LIMIT - 1) // GROUP_LIMIT
EXP_CAP = GROUPS * SLOT_PAIRS * TOKENS // EXPERTS


def draw_routes(route_key):
    key_hot, key_other, key_shift, key_cols = jax.random.split(route_key, 4)
    slot_sizes = [TOP // GROUP_LIMIT + int(slot_num < TOP % GROUP_LIMIT) for slot_num in range(GROUP_LIMIT)]
    slot_of_pair = jnp.array([slot_num for slot_num in range(GROUP_LIMIT) for step_num in range(slot_sizes[slot_num])], jnp.int32)
    step_of_pair = jnp.array([step_num for slot_num in range(GROUP_LIMIT) for step_num in range(slot_sizes[slot_num])], jnp.int32)
    hot_group = jax.random.randint(key_hot, (), 0, GROUPS).astype(jnp.int32)
    other_scores = jax.random.randint(key_other, (TOKENS, GROUPS - 1), 0, 1 << 20).astype(jnp.int32) * (GROUPS - 1) + jnp.arange(GROUPS - 1, dtype=jnp.int32)
    other_offsets = jnp.argsort(other_scores, axis=1)[:, : GROUP_LIMIT - 1].astype(jnp.int32)
    token_groups = jnp.concatenate([jnp.zeros((TOKENS, 1), jnp.int32) + hot_group, (hot_group + 1 + other_offsets) % GROUPS], axis=1)
    pair_groups = token_groups[:, slot_of_pair]
    group_shift = jax.random.randint(key_shift, (GROUPS,), 0, GROUP_WIDTH).astype(jnp.int32)
    token_pos = jnp.arange(TOKENS, dtype=jnp.int32)[:, None]
    within = (token_pos + step_of_pair[None, :] + group_shift[pair_groups]) % GROUP_WIDTH
    routes = pair_groups * GROUP_WIDTH + within
    col_scores = jax.random.randint(key_cols, (TOKENS, TOP), 0, 1 << 20).astype(jnp.int32) * TOP + jnp.arange(TOP, dtype=jnp.int32)
    col_order = jnp.argsort(col_scores, axis=1)
    return jnp.take_along_axis(routes, col_order, axis=1).astype(jnp.int32)


def setup_inputs(seed: int = 0, part: int = 0) -> dict:
    base_key = jax.random.key(seed)
    weight_keys = jax.random.split(base_key, 9)
    part_keys = jax.random.split(jax.random.fold_in(base_key, part), 2)
    hidden_in = jax.random.normal(part_keys[0], (TOKENS, D), jnp.float32).astype(jnp.bfloat16)
    expert_ids = draw_routes(part_keys[1])
    norm_gain = jax.random.uniform(weight_keys[0], (D,), jnp.float32, 0.5, 1.5)
    router_w = jax.random.normal(weight_keys[1], (EXPERTS, D), jnp.float32) * D ** -0.5
    w_gate = (jax.random.normal(weight_keys[2], (EXPERTS, D, INTER), jnp.float32) * D ** -0.5).astype(jnp.bfloat16)
    w_up = (jax.random.normal(weight_keys[3], (EXPERTS, D, INTER), jnp.float32) * D ** -0.5).astype(jnp.bfloat16)
    out_scale = jax.random.uniform(weight_keys[4], (EXPERTS, 1, 1), jnp.float32, 1.0, 3.0)
    w_down = (jax.random.normal(weight_keys[5], (EXPERTS, INTER, D), jnp.float32) * INTER ** -0.5 * out_scale).astype(jnp.bfloat16)
    ws_gate = (jax.random.normal(weight_keys[6], (D, SHARED_INTER), jnp.float32) * D ** -0.5).astype(jnp.bfloat16)
    ws_up = (jax.random.normal(weight_keys[7], (D, SHARED_INTER), jnp.float32) * D ** -0.5).astype(jnp.bfloat16)
    ws_down = (jax.random.normal(weight_keys[8], (SHARED_INTER, D), jnp.float32) * SHARED_INTER ** -0.5).astype(jnp.bfloat16)
    return {"hidden_in": hidden_in, "norm_gain": norm_gain, "router_w": router_w, "w_gate": w_gate, "w_up": w_up, "w_down": w_down, "ws_gate": ws_gate, "ws_up": ws_up, "ws_down": ws_down, "expert_ids": expert_ids}


def swiglu(tok_rows, gate_mat, up_mat, down_mat):
    h_gate = jnp.dot(tok_rows, gate_mat, preferred_element_type=jnp.float32)
    h_up = jnp.dot(tok_rows, up_mat, preferred_element_type=jnp.float32)
    hidden = (jax.nn.silu(h_gate) * h_up).astype(jnp.bfloat16)
    return jnp.dot(hidden, down_mat, preferred_element_type=jnp.float32).astype(jnp.bfloat16)


def reference(hidden_in, norm_gain, router_w, w_gate, w_up, w_down, ws_gate, ws_up, ws_down, expert_ids):
    x_f32 = hidden_in.astype(jnp.float32)
    inv_rms = lax.rsqrt(jnp.mean(x_f32 * x_f32, axis=1, keepdims=True) + NORM_EPS)
    x_norm = (x_f32 * inv_rms * norm_gain).astype(jnp.bfloat16)
    scores = jax.nn.sigmoid(jnp.dot(x_norm.astype(jnp.float32), router_w.T))
    picked = jnp.take_along_axis(scores, expert_ids, axis=1)
    gate_vals = ROUTE_SCALE * picked / jnp.sum(picked, axis=1, keepdims=True)
    flat_ids = expert_ids.reshape(-1)
    pair_tok = jnp.arange(TOKENS * TOP, dtype=jnp.int32) // TOP
    sort_order = jnp.argsort(flat_ids)
    counts = jnp.bincount(flat_ids, length=EXPERTS).astype(jnp.int32)
    starts = jnp.cumsum(counts) - counts
    sorted_tok = jnp.concatenate([pair_tok[sort_order], jnp.full((EXP_CAP,), TOKENS, jnp.int32)])
    norm_pad = jnp.concatenate([x_norm, jnp.zeros((1, D), x_norm.dtype)], axis=0)

    def one_expert(expert_xs):
        gate_mat, up_mat, down_mat, row_start, row_count = expert_xs
        row_tok = lax.dynamic_slice(sorted_tok, (row_start,), (EXP_CAP,))
        row_tok = jnp.where(jnp.arange(EXP_CAP, dtype=jnp.int32) < row_count, row_tok, TOKENS)
        return swiglu(norm_pad[row_tok], gate_mat, up_mat, down_mat)

    expert_out = lax.map(one_expert, (w_gate, w_up, w_down, starts, counts))
    sorted_rank = (jnp.arange(TOKENS * TOP, dtype=jnp.int32) - starts[flat_ids[sort_order]]).astype(jnp.int32)
    pair_rank = jnp.zeros((TOKENS * TOP,), jnp.int32).at[sort_order].set(sorted_rank)
    pair_out = expert_out[flat_ids, pair_rank].reshape(TOKENS, TOP, D)
    routed = jnp.sum(gate_vals[:, :, None] * pair_out.astype(jnp.float32), axis=1)
    shared_out = swiglu(x_norm, ws_gate, ws_up, ws_down)
    return (x_f32 + shared_out.astype(jnp.float32) + routed).astype(jnp.bfloat16)
```

```python
import functools
import math

import jax
import jax.numpy as jnp
from jax import lax
from jax.experimental import pallas as pl
from jax.experimental.pallas import tpu as pltpu
from jax.sharding import PartitionSpec as P

NORM_EPS = 1e-6
ROUTE_SCALE = 2.5
GROUPS = 8
GROUP_LIMIT = 4
MESH = pl.DeviceIdType.MESH
F32 = jnp.float32
BF16 = jnp.bfloat16
LINE = (0, -1, 1, 2)
CHUNKS = (
    ((0, 0), (1, 0), (-1, 0), (0, 1)),
    ((0, -1), (1, 1), (-1, 1), (1, -1)),
    ((-1, -1), (2, 0), (0, 2), (2, 1)),
    ((2, -1), (1, 2), (-1, 2), (2, 2)),
)
NT = (((1,), (1,)), ((), ()))


def split3(value):
    hi = value.astype(BF16)
    rest = value - hi.astype(F32)
    mid = rest.astype(BF16)
    lo = (rest - mid.astype(F32)).astype(BF16)
    return hi, mid, lo


def dot(a, b, dims=None):
    dims = (((1,), (0,)), ((), ())) if dims is None else dims
    return lax.dot_general(a, b, dims, preferred_element_type=F32)


def moe_kernel(
    side, cap,
    x_ref, gain_ref, router_ref, ids_ref, wg_hbm, wu_hbm, wd_hbm, sg_hbm, su_hbm, sd_hbm,
    out_ref, recv_hbm,
    wg, wu, wd, xall, xn, outb, xs, h, mask, acc, hs, meta, meta_in,
    w_sem, s_sem, ag_send, ag_recv, d2d_send, d2d_recv, meta_send, meta_recv, ret_send, ret_recv, load_sem,
):
    ep = 2 * side * side
    tok, dim = x_ref.shape
    inter = wg.shape[2]
    sinter = hs.shape[1]
    quarter = dim // 4
    lanes = meta.shape[2]
    nexp = router_ref.shape[0]
    me = lax.axis_index("ep")
    core = lax.rem(me, 2)
    chip = lax.div(me, 2)
    my_x = lax.rem(chip, side)
    my_y = lax.div(chip, side)

    def at_chip(dx, dy, dc=0):
        col = lax.rem(my_x + (dx + side), side)
        row = lax.rem(my_y + (dy + side), side)
        return (row * side + col) * 2 + (lax.rem(core + dc, 2) if dc else core)

    def at(half, da, db, dc=0):
        return at_chip(da, db, dc) if half == 0 else at_chip(db, da, dc)

    def rows(src, first, count):
        return xall.at[pl.ds(pl.multiple_of((src * 4 + first) * tok, tok), count * tok)]

    barrier = pltpu.get_barrier_semaphore()

    def greet(k, carry):
        pl.semaphore_signal(barrier, inc=1, device_id={"ep": lax.rem(me + k, ep)}, device_id_type=MESH)
        return carry

    lax.fori_loop(1, ep, greet, 0)
    weight_copies = []
    for i, (src, dst) in enumerate(((wg_hbm, wg), (wu_hbm, wu))):
        for e in range(2):
            weight_copies.append(pltpu.make_async_copy(src.at[e], dst.at[e], w_sem.at[i * 2 + e]))
    for e in range(2):
        weight_copies.append(
            pltpu.make_async_copy(wd_hbm.at[pl.ds(e * inter, inter)], wd.at[pl.ds(e * inter, inter)], w_sem.at[4 + e])
        )
    for copy in weight_copies:
        copy.start()

    x = x_ref[...].astype(F32)
    inv = lax.rsqrt(jnp.mean(x * x, axis=1, keepdims=True) + NORM_EPS)
    x_norm = (x * inv * gain_ref[...]).astype(BF16)
    xn[...] = x_norm
    base = pl.multiple_of(me * 4 * tok, tok)
    for q in range(4):
        xall[pl.ds(pl.multiple_of(base + q * tok, tok), tok), :] = x_norm[:, q * quarter : (q + 1) * quarter]

    ids = ids_ref[...]
    expert = lax.broadcasted_iota(jnp.int32, (nexp, lanes), 0)
    hot = expert == ids[0:1, :]
    top = 6
    for k in range(1, top):
        hot = jnp.logical_or(hot, expert == ids[k : k + 1, :])
    hot = jnp.where(hot, 1.0, 0.0)
    hot_b = hot.astype(BF16)
    upper = lax.broadcasted_iota(jnp.int32, (lanes, lanes), 0) < lax.broadcasted_iota(jnp.int32, (lanes, lanes), 1)
    before = dot(hot_b, jnp.where(upper, 1.0, 0.0).astype(BF16))
    e_row = lax.broadcasted_iota(jnp.int32, (nexp, nexp), 0)
    e_col = lax.broadcasted_iota(jnp.int32, (nexp, nexp), 1)
    same_dev = jnp.where(lax.shift_right_logical(e_row, 1) == lax.shift_right_logical(e_col, 1), 1.0, 0.0).astype(BF16)
    is_odd = jnp.bitwise_and(e_row, 1) == 1
    prev = jnp.where(jnp.logical_and(is_odd, e_col == e_row - 1), 1.0, 0.0).astype(BF16)
    rank = dot(same_dev, before.astype(BF16)) + dot(prev, hot_b)
    rank = jnp.where(hot > 0.5, rank, -1.0)
    r_hi, r_mid, r_lo = split3(router_ref[...])
    logits = dot(r_hi, x_norm, NT) + dot(r_mid, x_norm, NT) + dot(r_lo, x_norm, NT)
    picked = jnp.where(hot[:, :tok] > 0.5, jax.nn.sigmoid(logits), 0.0)
    gates = ROUTE_SCALE * picked / jnp.sum(picked, axis=0, keepdims=True)
    for d in range(ep):
        meta[d, 0:2, :] = rank[2 * d : 2 * d + 2, :]
        meta[d, 2:4, 0:tok] = gates[2 * d : 2 * d + 2, :]

    pl.semaphore_wait(barrier, ep - 1)

    sends = []

    def remote(src, dst, send_sem, recv_sem, target):
        return pltpu.make_async_remote_copy(
            src_ref=src, dst_ref=dst, send_sem=send_sem, recv_sem=recv_sem,
            device_id={"ep": target}, device_id_type=MESH,
        )

    def ag_copy(half, piece, block, first, count, target):
        remote(
            rows(block, first, count), rows(block, first, count), ag_send.at[half, piece], ag_recv.at[half, piece], target
        ).start()
        sends.append((ag_send, half, piece, count))

    def ag_wait(half, piece, block, first, count):
        remote(
            rows(block, first, count), rows(block, first, count), ag_send.at[half, piece], ag_recv.at[half, piece], at(half, 1, 0)
        ).wait_recv()

    def chip_slot(da, db, half):
        dx, dy = (da, db) if half == 0 else (db, da)
        return (dy % side) * side + dx % side

    def swap(half, da, db):
        block = at(half, da, db)
        view = rows(block, 2 * half, 2)
        slot = chip_slot(da, db, half)
        remote(view, view, d2d_send.at[half, slot], d2d_recv.at[half, slot], at_chip(0, 0, 1)).start()
        sends.append((d2d_send, half, slot, 2))

    def second_axis(half, line):
        block = at(half, LINE[line], 0)
        ag_copy(half, 4 + 2 * line, block, 2 * half, 2, at(half, 0, 1))
        ag_copy(half, 5 + 2 * line, block, 2 * half, 2, at(half, 0, -1))

    def first_arrived(half, way):
        off = (-1, 1)[way]
        block = at(half, off, 0)
        ag_wait(half, way, block, 2 * half, 2)
        ag_copy(half, 2 + way, block, 2 * half + way, 1, at(half, -off, 0))
        second_axis(half, 1 + way)
        swap(half, off, 0)

    def first_far_arrived(half):
        block = at(half, 2, 0)
        for way in range(2):
            ag_wait(half, 2 + way, block, 2 * half + way, 1)
        second_axis(half, 3)
        swap(half, 2, 0)

    def second_arrived(half, line, way):
        off = (-1, 1)[way]
        block = at(half, LINE[line], off)
        ag_wait(half, 4 + 2 * line + way, block, 2 * half, 2)
        ag_copy(half, 12 + 2 * line + way, block, 2 * half + way, 1, at(half, 0, -off))
        swap(half, LINE[line], off)

    def second_far_arrived(half, line):
        block = at(half, LINE[line], 2)
        for way in range(2):
            ag_wait(half, 12 + 2 * line + way, block, 2 * half + way, 1)
        swap(half, LINE[line], 2)

    for half in range(2):
        ag_copy(half, 0, me, 2 * half, 2, at(half, 1, 0))
        ag_copy(half, 1, me, 2 * half, 2, at(half, -1, 0))

    def meta_copy(k):
        target = lax.rem(me + k, ep)
        return remote(meta.at[target], meta_in.at[me], meta_send.at[k], meta_recv.at[me], target)

    def send_meta(k, carry):
        meta_copy(k).start()
        return carry

    for half in range(2):
        second_axis(half, 0)
    lax.fori_loop(1, ep, send_meta, 0)
    own_meta = pltpu.make_async_copy(meta.at[me], meta_in.at[me], meta_recv.at[me])
    own_meta.start()
    for half in range(2):
        swap(half, 0, 0)
    for half in range(2):
        for way in range(2):
            first_arrived(half, way)
    for half in range(2):
        for way in range(2):
            second_arrived(half, 0, way)

    def events(*calls):
        return calls

    gate_events = (
        events((first_far_arrived, 0), (first_far_arrived, 1)),
        events((second_arrived, 0, 1, 0), (second_arrived, 1, 1, 0), (second_arrived, 0, 1, 1), (second_arrived, 1, 1, 1)),
        events((second_arrived, 0, 2, 0), (second_arrived, 1, 2, 0), (second_arrived, 0, 2, 1), (second_arrived, 1, 2, 1)),
        events((second_far_arrived, 0, 0), (second_far_arrived, 1, 0)),
        events((second_arrived, 0, 3, 0), (second_arrived, 1, 3, 0), (second_arrived, 0, 3, 1), (second_arrived, 1, 3, 1)),
    )
    down_events = (
        events((second_far_arrived, 0, 1), (second_far_arrived, 1, 1)),
        events((second_far_arrived, 0, 2), (second_far_arrived, 1, 2)),
        events((second_far_arrived, 0, 3), (second_far_arrived, 1, 3)),
    )

    tile = 256
    per = 2 * len(CHUNKS[0])
    full, left = inter // tile, inter % tile
    down_tiles = dim // tile

    def chunk_device(c, j):
        return (*CHUNKS[c][j // 2], j % 2)

    def wait_meta(src):
        remote(meta.at[0], meta_in.at[src], meta_send.at[1], meta_recv.at[src], src).wait_recv()

    def select(c):
        slot_no = lax.broadcasted_iota(jnp.int32, (cap, tok), 0).astype(F32)
        for j in range(per):
            dx, dy, dc = chunk_device(c, j)
            src = at_chip(dx, dy, dc)
            if (dx, dy, dc) == (0, 0, 0):
                own_meta.wait()
            else:
                wait_meta(src)
            if dc:
                for half in range(2):
                    slot = (dy % side) * side + dx % side
                    view = rows(src, 2 * half, 2)
                    remote(view, view, d2d_send.at[half, slot], d2d_recv.at[half, slot], at_chip(0, 0, 1)).wait_recv()
            low = jnp.where(slot_no == meta_in[src, 0:1, 0:tok], 1.0, 0.0)
            high = jnp.where(slot_no == meta_in[src, 1:2, 0:tok], 1.0, 0.0)
            mask[j * cap : (j + 1) * cap, :] = jnp.broadcast_to(jnp.sum(low, axis=1, keepdims=True), (cap, tile))
            pick = (low + high).astype(BF16)
            for q in range(4):
                block = xall[pl.ds(pl.multiple_of((src * 4 + q) * tok, tok), tok), :]
                xs[j * cap : (j + 1) * cap, q * quarter : (q + 1) * quarter] = dot(pick, block).astype(BF16)

    def gated(gate, up, is_low, keep_low):
        keep = is_low > 0.5
        keep = keep if keep_low else jnp.logical_not(keep)
        return jnp.where(keep, jax.nn.silu(gate) * up, 0.0).astype(BF16)

    def gate_up(n, carry):
        cols = pl.ds(pl.multiple_of(n * tile, tile), tile)
        for e in range(2):
            gate = dot(xs[...], wg[e, :, cols])
            up = dot(xs[...], wu[e, :, cols])
            h[:, pl.ds(pl.multiple_of(e * inter + n * tile, 128), tile)] = gated(gate, up, mask[...], e == 0)
        return carry

    def gate_up_left():
        cols = slice(full * tile, inter)
        for e in range(2):
            both = dot(xs[...], jnp.concatenate([wg[e, :, cols], wu[e, :, cols]], axis=1))
            h[:, e * inter + full * tile : (e + 1) * inter] = gated(both[:, :left], both[:, left:], mask[:, :left], e == 0)

    def down(c, n):
        cols = pl.ds(pl.multiple_of(n * tile, tile), tile)
        y = dot(h[...], wd[:, cols]).astype(BF16)
        outb[c * per : (c + 1) * per, :, cols] = y.reshape(per, cap, tile)

    def run_events(n, table):
        for k, calls in enumerate(table):
            if calls:

                @pl.when(n == k)
                def _():
                    for fn, *args in calls:
                        fn(*args)

    ret_copies = []

    def send_back(c):
        for j in range(per):
            dx, dy, dc = chunk_device(c, j)
            block = outb.at[c * per + j]
            if (dx, dy, dc) == (0, 0, 0):
                copy = pltpu.make_async_copy(block, recv_hbm.at[me], ret_recv.at[me])
            else:
                copy = remote(block, recv_hbm.at[me], ret_send.at[c * per + j], ret_recv.at[me], at_chip(dx, dy, dc))
            copy.start()
            ret_copies.append(copy)

    for c in range(len(CHUNKS)):
        select(c)
        if c > 0:
            send_back(c - 1)
        if c == 0:
            for copy in weight_copies[:4]:
                copy.wait()

        def gate_step(n, carry, c=c):
            gate_up(n, 0)
            if c == 0:
                run_events(n, gate_events)
            return carry

        lax.fori_loop(0, full, gate_step, 0)
        if left:
            gate_up_left()
        if c == 0:
            for copy in weight_copies[4:]:
                copy.wait()

        def down_step(n, carry, c=c):
            down(c, n)
            if c == 0:
                run_events(n, down_events)
            return carry

        lax.fori_loop(0, down_tiles, down_step, 0)

    for sems, half, i, count in sends:
        view = rows(me, 0, count)
        remote(view, view, sems.at[half, i], ag_recv.at[0, 0], at_chip(0, 0, 1)).wait_send()
    s_tile = quarter
    s_steps = [(n * s_tile, min(s_tile, sinter - n * s_tile)) for n in range(-(-sinter // s_tile))]
    pair_slots = xall.shape[0] // (2 * dim)
    pairs = []
    for n, (col, width) in enumerate(s_steps):
        top_row = (n % pair_slots) * 2 * dim
        views = [xall.at[pl.ds(top_row + i * dim, dim), pl.ds(0, width)] for i in range(2)]
        pairs.append([
            pltpu.make_async_copy(w.at[:, pl.ds(col, width)], views[i], s_sem.at[2 * (n % pair_slots) + i])
            for i, w in enumerate((sg_hbm, su_hbm))
        ])
    downs = [
        pltpu.make_async_copy(
            sd_hbm.at[:, pl.ds(n * s_tile, s_tile)], xall.at[pl.ds(n * sinter, sinter), :], s_sem.at[2 * pair_slots + n]
        )
        for n in range(4)
    ]
    for n in range(min(pair_slots, len(pairs))):
        for copy in pairs[n]:
            copy.start()
    send_back(len(CHUNKS) - 1)

    started = 0
    for n, (col, width) in enumerate(s_steps):
        for copy in pairs[n]:
            copy.wait()
        top_row = (n % pair_slots) * 2 * dim
        gate = dot(xn[...], xall[top_row : top_row + dim, 0:width])
        up = dot(xn[...], xall[top_row + dim : top_row + 2 * dim, 0:width])
        hs[:, col : col + width] = (jax.nn.silu(gate) * up).astype(BF16)
        if n + pair_slots < len(pairs):
            for copy in pairs[n + pair_slots]:
                copy.start()
        busy = [(m % pair_slots) * 2 * dim for m in range(n + 1, min(n + 1 + pair_slots, len(pairs)))]
        while started < 4 and all(
            (started + 1) * sinter <= b or started * sinter >= b + 2 * dim for b in busy
        ):
            if n + pair_slots < len(pairs):
                break
            downs[started].start()
            started += 1
    for n in range(4):
        downs[n].wait()
        cols = slice(n * s_tile, (n + 1) * s_tile)
        y = dot(hs[...], xall[n * sinter : (n + 1) * sinter, :]).astype(BF16)
        acc[:, cols] = x_ref[:, cols].astype(F32) + y.astype(F32)

    for c in range(len(CHUNKS)):
        loads = []
        weights = []
        slot_no = lax.broadcasted_iota(jnp.int32, (cap, lanes), 0).astype(F32)
        for j in range(per):
            dx, dy, dc = chunk_device(c, j)
            dev = at_chip(-dx, -dy, dc)
            if (dx, dy, dc) == (0, 0, 0):
                ret_copies[0].wait()
            else:
                remote(outb.at[0], recv_hbm.at[dev], ret_send.at[1], ret_recv.at[dev], dev).wait_recv()
            load = pltpu.make_async_copy(recv_hbm.at[dev], xs.at[pl.ds(j * cap, cap)], load_sem.at[j])
            load.start()
            loads.append(load)
            valid = lax.broadcasted_iota(jnp.int32, (1, lanes), 1) < tok
            low = jnp.where(slot_no == meta[dev, 0:1, :], jnp.where(valid, meta[dev, 2:3, :], 0.0), 0.0)
            high = jnp.where(slot_no == meta[dev, 1:2, :], jnp.where(valid, meta[dev, 3:4, :], 0.0), 0.0)
            weights.append(low + high)
        w_all = jnp.concatenate(weights, axis=0).T
        parts = [p[:tok] for p in split3(w_all)]
        for load in loads:
            load.wait()
        for q in range(4):
            cols = slice(q * quarter, (q + 1) * quarter)
            block = xs[:, cols]
            part = dot(parts[0], block) + dot(parts[1], block) + dot(parts[2], block)
            total = acc[:, cols] + part
            if c == len(CHUNKS) - 1:
                out_ref[:, cols] = total.astype(BF16)
            else:
                acc[:, cols] = total

    def meta_sent(k, carry):
        meta_copy(k).wait_send()
        return carry

    lax.fori_loop(1, ep, meta_sent, 0)
    for copy in ret_copies[1:]:
        copy.wait_send()


def solution(mesh):
    ep_size = mesh.shape["ep"]
    side = math.isqrt(ep_size // 2)

    def local_block(hidden_in, norm_gain, router_w, w_gate, w_up, w_down, ws_gate, ws_up, ws_down, expert_ids):
        tok, top_k = expert_ids.shape
        dim = hidden_in.shape[1]
        exp_dev, _, inter = w_gate.shape
        sinter = ws_gate.shape[1]
        cap = GROUPS * ((top_k + GROUP_LIMIT - 1) // GROUP_LIMIT) * tok // ep_size
        lanes = 128
        ids = jnp.pad(expert_ids.T, ((0, 8 - top_k), (0, lanes - tok)), constant_values=-1)
        chunk_rows = cap * 8
        any_spec = pl.BlockSpec(memory_space=pl.ANY)
        vmem_spec = pl.BlockSpec(memory_space=pltpu.VMEM)
        out, _ = pl.pallas_call(
            functools.partial(moe_kernel, side, cap),
            out_shape=(
                jax.ShapeDtypeStruct((tok, dim), BF16),
                jax.ShapeDtypeStruct((ep_size, cap, dim), BF16),
            ),
            in_specs=[vmem_spec] * 4 + [any_spec] * 6,
            out_specs=(vmem_spec, any_spec),
            scratch_shapes=[
                pltpu.VMEM((exp_dev, dim, inter), BF16),
                pltpu.VMEM((exp_dev, dim, inter), BF16),
                pltpu.VMEM((exp_dev * inter, dim), BF16),
                pltpu.VMEM((ep_size * 4 * tok, dim // 4), BF16),
                pltpu.VMEM((tok, dim), BF16),
                pltpu.VMEM((ep_size, cap, dim), BF16),
                pltpu.VMEM((chunk_rows, dim), BF16),
                pltpu.VMEM((chunk_rows, exp_dev * inter), BF16),
                pltpu.VMEM((chunk_rows, 256), F32),
                pltpu.VMEM((tok, dim), F32),
                pltpu.VMEM((tok, sinter), BF16),
                pltpu.VMEM((ep_size, 8, lanes), F32),
                pltpu.VMEM((ep_size, 8, lanes), F32),
                pltpu.SemaphoreType.DMA((6,)),
                pltpu.SemaphoreType.DMA((32,)),
                pltpu.SemaphoreType.DMA((2, 20)),
                pltpu.SemaphoreType.DMA((2, 20)),
                pltpu.SemaphoreType.DMA((2, side * side)),
                pltpu.SemaphoreType.DMA((2, side * side)),
                pltpu.SemaphoreType.DMA((ep_size,)),
                pltpu.SemaphoreType.DMA((ep_size,)),
                pltpu.SemaphoreType.DMA((ep_size,)),
                pltpu.SemaphoreType.DMA((ep_size,)),
                pltpu.SemaphoreType.DMA((8,)),
            ],
            compiler_params=pltpu.CompilerParams(
                collective_id=0, has_side_effects=True, vmem_limit_bytes=67_000_000
            ),
        )(
            hidden_in, norm_gain.reshape(1, dim), router_w, ids, w_gate, w_up,
            w_down.reshape(exp_dev * inter, dim), ws_gate, ws_up, ws_down,
        )
        return out

    row_spec = P(("dp", "ep"), None)
    in_specs = (row_spec, P(), P(), P("ep"), P("ep"), P("ep"), P(), P(), P(), row_spec)
    return jax.shard_map(local_block, mesh=mesh, in_specs=in_specs, out_specs=row_spec, check_vma=False)
```

```python
import functools
import math

import jax
import jax.numpy as jnp
from jax import lax
from jax.experimental import pallas as pl
from jax.experimental.pallas import tpu as pltpu
from jax.sharding import PartitionSpec as P

NORM_EPS = 1e-6
ROUTE_SCALE = 2.5
GROUPS = 8
GROUP_LIMIT = 4
MESH = pl.DeviceIdType.MESH
F32 = jnp.float32
BF16 = jnp.bfloat16
LINE = (0, -1, 1, 2)
CHUNKS = (
    ((0, 0), (1, 0), (-1, 0), (2, 0)),
    ((0, -1), (0, 1), (1, -1), (-1, 1)),
    ((0, 2), (1, 2), (-1, 2), (2, 2)),
    ((-1, -1), (1, 1), (2, -1), (2, 1)),
)
NT = (((1,), (1,)), ((), ()))


def split3(value):
    hi = value.astype(BF16)
    rest = value - hi.astype(F32)
    mid = rest.astype(BF16)
    lo = (rest - mid.astype(F32)).astype(BF16)
    return hi, mid, lo


def dot(a, b, dims=None):
    dims = (((1,), (0,)), ((), ())) if dims is None else dims
    return lax.dot_general(a, b, dims, preferred_element_type=F32)


def moe_kernel(
    side, cap,
    x_ref, gain_ref, router_ref, ids_ref, wg_hbm, wu_hbm, wd_hbm, sg_hbm, su_hbm, sd_hbm,
    out_ref, recv_hbm,
    wg, wu, wd, xall, xn, outb, xs, h, mask, acc, hs, meta, meta_in,
    w_sem, s_sem, ag_send, ag_recv, d2d_send, d2d_recv, meta_send, meta_recv, ret_send, ret_recv, load_sem,
):
    ep = 2 * side * side
    tok, dim = x_ref.shape
    inter = wg.shape[2]
    sinter = hs.shape[1]
    quarter = dim // 4
    lanes = meta.shape[2]
    nexp = router_ref.shape[0]
    me = lax.axis_index("ep")
    core = lax.rem(me, 2)
    chip = lax.div(me, 2)
    my_x = lax.rem(chip, side)
    my_y = lax.div(chip, side)

    peer = me + 1 - 2 * core

    def at(first, second, plane=core, dev_core=None):
        col = lax.rem(my_x + side + second + plane * (first - second), side)
        row = lax.rem(my_y + side + first + plane * (second - first), side)
        return (row * side + col) * 2 + (plane if dev_core is None else dev_core)

    def rows(src, first, count):
        return xall.at[pl.ds(pl.multiple_of((src * 4 + first) * tok, tok), count * tok)]

    barrier = pltpu.get_barrier_semaphore()

    def greet(k, carry):
        pl.semaphore_signal(barrier, inc=1, device_id={"ep": lax.rem(me + k, ep)}, device_id_type=MESH)
        return carry

    lax.fori_loop(1, ep, greet, 0)
    weight_copies = []
    for i, (src, dst) in enumerate(((wg_hbm, wg), (wu_hbm, wu))):
        for e in range(2):
            weight_copies.append(pltpu.make_async_copy(src.at[e], dst.at[e], w_sem.at[i * 2 + e]))
    for e in range(2):
        weight_copies.append(
            pltpu.make_async_copy(wd_hbm.at[pl.ds(e * inter, inter)], wd.at[pl.ds(e * inter, inter)], w_sem.at[4 + e])
        )
    for copy in weight_copies:
        copy.start()

    x = x_ref[...].astype(F32)
    inv = lax.rsqrt(jnp.mean(x * x, axis=1, keepdims=True) + NORM_EPS)
    x_norm = (x * inv * gain_ref[...]).astype(BF16)
    xn[...] = x_norm
    base = pl.multiple_of(me * 4 * tok, tok)
    for q in range(4):
        xall[pl.ds(pl.multiple_of(base + q * tok, tok), tok), :] = x_norm[:, q * quarter : (q + 1) * quarter]

    pl.semaphore_wait(barrier, ep - 1)

    sends = []

    def remote(src, dst, send_sem, recv_sem, target):
        return pltpu.make_async_remote_copy(
            src_ref=src, dst_ref=dst, send_sem=send_sem, recv_sem=recv_sem,
            device_id={"ep": target}, device_id_type=MESH,
        )

    def ag_copy(piece, block, first, count, target):
        view = rows(block, first, count)
        remote(view, view, ag_send.at[piece], ag_recv.at[piece], target).start()
        sends.append((ag_send, piece, count))

    def ag_wait(piece, block, first, count):
        view = rows(block, first, count)
        remote(view, view, ag_send.at[piece], ag_recv.at[piece], at(1, 0)).wait_recv()

    def swap(first, second):
        view = rows(at(first, second), 0, 4)
        slot = (first % side) * side + second % side
        remote(view, view, d2d_send.at[slot], d2d_recv.at[slot], peer).start()
        sends.append((d2d_send, slot, 4))

    def second_axis(line):
        block = at(LINE[line], 0)
        ag_copy(4 + 2 * line, block, 0, 4, at(0, 1))
        ag_copy(5 + 2 * line, block, 0, 4, at(0, -1))

    def first_arrived(way):
        off = (-1, 1)[way]
        block = at(off, 0)
        ag_wait(way, block, 0, 4)
        ag_copy(2 + way, block, 2 * way, 2, at(-off, 0))

    def first_far_arrived():
        block = at(2, 0)
        for way in range(2):
            ag_wait(2 + way, block, 2 * way, 2)
        swap(2, 0)
        second_axis(3)

    def second_arrived(line, way):
        off = (-1, 1)[way]
        block = at(LINE[line], off)
        ag_wait(4 + 2 * line + way, block, 0, 4)
        ag_copy(12 + 2 * line + way, block, 2 * way, 2, at(0, -off))
        swap(LINE[line], off)

    def second_far_arrived(line):
        block = at(LINE[line], 2)
        for way in range(2):
            ag_wait(12 + 2 * line + way, block, 2 * way, 2)
        swap(LINE[line], 2)

    ag_copy(0, me, 0, 4, at(1, 0))
    ag_copy(1, me, 0, 4, at(-1, 0))
    swap(0, 0)

    ids = ids_ref[...]
    expert = lax.broadcasted_iota(jnp.int32, (nexp, lanes), 0)
    hot = expert == ids[0:1, :]
    top = 6
    for k in range(1, top):
        hot = jnp.logical_or(hot, expert == ids[k : k + 1, :])
    hot = jnp.where(hot, 1.0, 0.0)
    hot_b = hot.astype(BF16)
    upper = lax.broadcasted_iota(jnp.int32, (lanes, lanes), 0) < lax.broadcasted_iota(jnp.int32, (lanes, lanes), 1)
    before = dot(hot_b, jnp.where(upper, 1.0, 0.0).astype(BF16))
    e_row = lax.broadcasted_iota(jnp.int32, (nexp, nexp), 0)
    e_col = lax.broadcasted_iota(jnp.int32, (nexp, nexp), 1)
    same_dev = jnp.where(lax.shift_right_logical(e_row, 1) == lax.shift_right_logical(e_col, 1), 1.0, 0.0).astype(BF16)
    is_odd = jnp.bitwise_and(e_row, 1) == 1
    prev = jnp.where(jnp.logical_and(is_odd, e_col == e_row - 1), 1.0, 0.0).astype(BF16)
    rank = dot(same_dev, before.astype(BF16)) + dot(prev, hot_b)
    rank = jnp.where(hot > 0.5, rank, -1.0)
    r_hi, r_mid, r_lo = split3(router_ref[...])
    logits = dot(r_hi, x_norm, NT) + dot(r_mid, x_norm, NT) + dot(r_lo, x_norm, NT)
    picked = jnp.where(hot[:, :tok] > 0.5, jax.nn.sigmoid(logits), 0.0)
    gates = ROUTE_SCALE * picked / jnp.sum(picked, axis=0, keepdims=True)
    for d in range(ep):
        meta[d, 0:2, :] = rank[2 * d : 2 * d + 2, :]
        meta[d, 2:4, 0:tok] = gates[2 * d : 2 * d + 2, :]

    def meta_copy(k):
        target = lax.rem(me + k, ep)
        return remote(meta.at[target], meta_in.at[me], meta_send.at[k], meta_recv.at[me], target)

    def send_meta(k, carry):
        meta_copy(k).start()
        return carry

    first_arrived(0)
    first_arrived(1)
    lax.fori_loop(1, ep, send_meta, 0)
    own_meta = pltpu.make_async_copy(meta.at[me], meta_in.at[me], meta_recv.at[me])
    own_meta.start()
    second_axis(0)
    for way in range(2):
        swap((-1, 1)[way], 0)
        second_axis(1 + way)
    first_far_arrived()

    gate_events = (
        ((), ((second_arrived, 0, 0), (second_arrived, 0, 1)), ((second_arrived, 1, 0), (second_arrived, 1, 1)), (), ((second_arrived, 2, 0), (second_arrived, 2, 1))),
        (((second_far_arrived, 0),), ((second_far_arrived, 1),), ((second_far_arrived, 2),), ((second_far_arrived, 3),)),
    )
    down_events = (((),) * 5 + (((second_arrived, 3, 0), (second_arrived, 3, 1)),), ())

    tile = 256
    per = 2 * len(CHUNKS[0])
    full, left = inter // tile, inter % tile
    down_tiles = dim // tile

    def source(c, j):
        first, second = CHUNKS[c][j % (per // 2)]
        return at(first, second, core if j < per // 2 else 1 - core)

    def wait_meta(src):
        remote(meta.at[0], meta_in.at[src], meta_send.at[1], meta_recv.at[src], src).wait_recv()

    def select(c):
        slot_no = lax.broadcasted_iota(jnp.int32, (cap, tok), 0).astype(F32)
        for j in range(per):
            src = source(c, j)
            if c == 0 and j == 0:
                own_meta.wait()
            else:
                wait_meta(src)
            if j >= per // 2:
                first, second = CHUNKS[c][j % (per // 2)]
                slot = (first % side) * side + second % side
                view = rows(src, 0, 4)
                remote(view, view, d2d_send.at[slot], d2d_recv.at[slot], peer).wait_recv()
            low = jnp.where(slot_no == meta_in[src, 0:1, 0:tok], 1.0, 0.0)
            high = jnp.where(slot_no == meta_in[src, 1:2, 0:tok], 1.0, 0.0)
            mask[j * cap : (j + 1) * cap, :] = jnp.broadcast_to(jnp.sum(low, axis=1, keepdims=True), (cap, tile))
            pick = (low + high).astype(BF16)
            for q in range(4):
                block = xall[pl.ds(pl.multiple_of((src * 4 + q) * tok, tok), tok), :]
                xs[j * cap : (j + 1) * cap, q * quarter : (q + 1) * quarter] = dot(pick, block).astype(BF16)

    def gated(gate, up, is_low, keep_low):
        keep = is_low > 0.5
        keep = keep if keep_low else jnp.logical_not(keep)
        return jnp.where(keep, jax.nn.silu(gate) * up, 0.0).astype(BF16)

    def gate_up(n, carry):
        cols = pl.ds(pl.multiple_of(n * tile, tile), tile)
        for e in range(2):
            gate = dot(xs[...], wg[e, :, cols])
            up = dot(xs[...], wu[e, :, cols])
            h[:, pl.ds(pl.multiple_of(e * inter + n * tile, 128), tile)] = gated(gate, up, mask[...], e == 0)
        return carry

    def gate_up_left():
        cols = slice(full * tile, inter)
        for e in range(2):
            both = dot(xs[...], jnp.concatenate([wg[e, :, cols], wu[e, :, cols]], axis=1))
            h[:, e * inter + full * tile : (e + 1) * inter] = gated(both[:, :left], both[:, left:], mask[:, :left], e == 0)

    def down(c, n):
        cols = pl.ds(pl.multiple_of(n * tile, tile), tile)
        y = dot(h[...], wd[:, cols]).astype(BF16)
        outb[c * per : (c + 1) * per, :, cols] = y.reshape(per, cap, tile)

    def run_events(n, table):
        for k, calls in enumerate(table):
            if calls:

                @pl.when(n == k)
                def _():
                    for fn, *args in calls:
                        fn(*args)

    ret_copies = []

    def send_back(c):
        for j in range(per):
            block = outb.at[c * per + j]
            if c == 0 and j == 0:
                copy = pltpu.make_async_copy(block, recv_hbm.at[me], ret_recv.at[me])
            else:
                copy = remote(block, recv_hbm.at[me], ret_send.at[c * per + j], ret_recv.at[me], source(c, j))
            copy.start()
            ret_copies.append(copy)

    for c in range(len(CHUNKS)):
        select(c)
        if c > 0:
            send_back(c - 1)
        if c == 0:
            for copy in weight_copies[:4]:
                copy.wait()

        def gate_step(n, carry, c=c):
            gate_up(n, 0)
            if c < len(gate_events):
                run_events(n, gate_events[c])
            return carry

        lax.fori_loop(0, full, gate_step, 0)
        if left:
            gate_up_left()
        if c == 0:
            for copy in weight_copies[4:]:
                copy.wait()

        def down_step(n, carry, c=c):
            down(c, n)
            if c < len(down_events):
                run_events(n, down_events[c])
            return carry

        lax.fori_loop(0, down_tiles, down_step, 0)

    for sems, i, count in sends:
        view = rows(me, 0, count)
        remote(view, view, sems.at[i], ag_recv.at[0], peer).wait_send()
    s_tile = quarter
    s_steps = [(n * s_tile, min(s_tile, sinter - n * s_tile)) for n in range(-(-sinter // s_tile))]
    pair_slots = xall.shape[0] // (2 * dim)
    pairs = []
    for n, (col, width) in enumerate(s_steps):
        top_row = (n % pair_slots) * 2 * dim
        views = [xall.at[pl.ds(top_row + i * dim, dim), pl.ds(0, width)] for i in range(2)]
        pairs.append([
            pltpu.make_async_copy(w.at[:, pl.ds(col, width)], views[i], s_sem.at[2 * (n % pair_slots) + i])
            for i, w in enumerate((sg_hbm, su_hbm))
        ])
    downs = [
        pltpu.make_async_copy(
            sd_hbm.at[:, pl.ds(n * s_tile, s_tile)], xall.at[pl.ds(n * sinter, sinter), :], s_sem.at[2 * pair_slots + n]
        )
        for n in range(4)
    ]
    for n in range(min(pair_slots, len(pairs))):
        for copy in pairs[n]:
            copy.start()
    send_back(len(CHUNKS) - 1)

    started = 0
    for n, (col, width) in enumerate(s_steps):
        for copy in pairs[n]:
            copy.wait()
        top_row = (n % pair_slots) * 2 * dim
        gate = dot(xn[...], xall[top_row : top_row + dim, 0:width])
        up = dot(xn[...], xall[top_row + dim : top_row + 2 * dim, 0:width])
        hs[:, col : col + width] = (jax.nn.silu(gate) * up).astype(BF16)
        if n + pair_slots < len(pairs):
            for copy in pairs[n + pair_slots]:
                copy.start()
        busy = [(m % pair_slots) * 2 * dim for m in range(n + 1, min(n + 1 + pair_slots, len(pairs)))]
        while started < 4 and all(
            (started + 1) * sinter <= b or started * sinter >= b + 2 * dim for b in busy
        ):
            if n + pair_slots < len(pairs):
                break
            downs[started].start()
            started += 1
    for n in range(4):
        downs[n].wait()
        cols = slice(n * s_tile, (n + 1) * s_tile)
        y = dot(hs[...], xall[n * sinter : (n + 1) * sinter, :]).astype(BF16)
        acc[:, cols] = x_ref[:, cols].astype(F32) + y.astype(F32)

    for c in range(len(CHUNKS)):
        loads = []
        weights = []
        slot_no = lax.broadcasted_iota(jnp.int32, (cap, lanes), 0).astype(F32)
        for j in range(per):
            first, second = CHUNKS[c][j % (per // 2)]
            dev = at(-first, -second, core, core if j < per // 2 else 1 - core)
            if c == 0 and j == 0:
                ret_copies[0].wait()
            else:
                remote(outb.at[0], recv_hbm.at[dev], ret_send.at[1], ret_recv.at[dev], dev).wait_recv()
            load = pltpu.make_async_copy(recv_hbm.at[dev], xs.at[pl.ds(j * cap, cap)], load_sem.at[j])
            load.start()
            loads.append(load)
            valid = lax.broadcasted_iota(jnp.int32, (1, lanes), 1) < tok
            low = jnp.where(slot_no == meta[dev, 0:1, :], jnp.where(valid, meta[dev, 2:3, :], 0.0), 0.0)
            high = jnp.where(slot_no == meta[dev, 1:2, :], jnp.where(valid, meta[dev, 3:4, :], 0.0), 0.0)
            weights.append(low + high)
        w_all = jnp.concatenate(weights, axis=0).T
        parts = [p[:tok] for p in split3(w_all)]
        for load in loads:
            load.wait()
        for q in range(4):
            cols = slice(q * quarter, (q + 1) * quarter)
            block = xs[:, cols]
            part = dot(parts[0], block) + dot(parts[1], block) + dot(parts[2], block)
            total = acc[:, cols] + part
            if c == len(CHUNKS) - 1:
                out_ref[:, cols] = total.astype(BF16)
            else:
                acc[:, cols] = total

    def meta_sent(k, carry):
        meta_copy(k).wait_send()
        return carry

    lax.fori_loop(1, ep, meta_sent, 0)
    for copy in ret_copies[1:]:
        copy.wait_send()


def solution(mesh):
    ep_size = mesh.shape["ep"]
    side = math.isqrt(ep_size // 2)

    def local_block(hidden_in, norm_gain, router_w, w_gate, w_up, w_down, ws_gate, ws_up, ws_down, expert_ids):
        tok, top_k = expert_ids.shape
        dim = hidden_in.shape[1]
        exp_dev, _, inter = w_gate.shape
        sinter = ws_gate.shape[1]
        cap = GROUPS * ((top_k + GROUP_LIMIT - 1) // GROUP_LIMIT) * tok // ep_size
        lanes = 128
        ids = jnp.pad(expert_ids.T, ((0, 8 - top_k), (0, lanes - tok)), constant_values=-1)
        chunk_rows = cap * 8
        any_spec = pl.BlockSpec(memory_space=pl.ANY)
        vmem_spec = pl.BlockSpec(memory_space=pltpu.VMEM)
        out, _ = pl.pallas_call(
            functools.partial(moe_kernel, side, cap),
            out_shape=(
                jax.ShapeDtypeStruct((tok, dim), BF16),
                jax.ShapeDtypeStruct((ep_size, cap, dim), BF16),
            ),
            in_specs=[vmem_spec] * 4 + [any_spec] * 6,
            out_specs=(vmem_spec, any_spec),
            scratch_shapes=[
                pltpu.VMEM((exp_dev, dim, inter), BF16),
                pltpu.VMEM((exp_dev, dim, inter), BF16),
                pltpu.VMEM((exp_dev * inter, dim), BF16),
                pltpu.VMEM((ep_size * 4 * tok, dim // 4), BF16),
                pltpu.VMEM((tok, dim), BF16),
                pltpu.VMEM((ep_size, cap, dim), BF16),
                pltpu.VMEM((chunk_rows, dim), BF16),
                pltpu.VMEM((chunk_rows, exp_dev * inter), BF16),
                pltpu.VMEM((chunk_rows, 256), F32),
                pltpu.VMEM((tok, dim), F32),
                pltpu.VMEM((tok, sinter), BF16),
                pltpu.VMEM((ep_size, 8, lanes), F32),
                pltpu.VMEM((ep_size, 8, lanes), F32),
                pltpu.SemaphoreType.DMA((6,)),
                pltpu.SemaphoreType.DMA((32,)),
                pltpu.SemaphoreType.DMA((20,)),
                pltpu.SemaphoreType.DMA((20,)),
                pltpu.SemaphoreType.DMA((side * side,)),
                pltpu.SemaphoreType.DMA((side * side,)),
                pltpu.SemaphoreType.DMA((ep_size,)),
                pltpu.SemaphoreType.DMA((ep_size,)),
                pltpu.SemaphoreType.DMA((ep_size,)),
                pltpu.SemaphoreType.DMA((ep_size,)),
                pltpu.SemaphoreType.DMA((8,)),
            ],
            compiler_params=pltpu.CompilerParams(
                collective_id=0, has_side_effects=True, vmem_limit_bytes=67_000_000
            ),
        )(
            hidden_in, norm_gain.reshape(1, dim), router_w, ids, w_gate, w_up,
            w_down.reshape(exp_dev * inter, dim), ws_gate, ws_up, ws_down,
        )
        return out

    row_spec = P(("dp", "ep"), None)
    in_specs = (row_spec, P(), P(), P("ep"), P("ep"), P("ep"), P(), P(), P(), row_spec)
    return jax.shard_map(local_block, mesh=mesh, in_specs=in_specs, out_specs=row_spec, check_vma=False)
```

```python
import functools
import math

import jax
import jax.numpy as jnp
from jax import lax
from jax.experimental import pallas as pl
from jax.experimental.pallas import tpu as pltpu
from jax.sharding import PartitionSpec as P

NORM_EPS = 1e-6
ROUTE_SCALE = 2.5
GROUPS = 8
GROUP_LIMIT = 4
MESH = pl.DeviceIdType.MESH
F32 = jnp.float32
BF16 = jnp.bfloat16
LINE = (0, -1, 1, 2)
CHUNKS = (
    ((0, 0), (1, 0)),
    ((-1, 0), (2, 0)),
    ((-1, -1), (1, 1)),
    ((2, -1), (2, 1)),
    ((1, 2), (-1, 2)),
    ((0, 2), (2, 2)),
    ((1, -1), (-1, 1)),
    ((0, -1), (0, 1)),
)
NT = (((1,), (1,)), ((), ()))


def split3(value):
    hi = value.astype(BF16)
    rest = value - hi.astype(F32)
    mid = rest.astype(BF16)
    lo = (rest - mid.astype(F32)).astype(BF16)
    return hi, mid, lo


def dot(a, b, dims=None):
    dims = (((1,), (0,)), ((), ())) if dims is None else dims
    return lax.dot_general(a, b, dims, preferred_element_type=F32)


def moe_kernel(
    side, cap,
    x_ref, gain_ref, router_ref, ids_ref, wg_hbm, wu_hbm, wd_hbm, sg_hbm, su_hbm, sd_hbm,
    out_ref, recv_hbm,
    wg, wu, wd, xall, xn, outb, xs, h, mask, acc, hs, mix, meta, meta_in,
    w_sem, s_sem, ag_send, ag_recv, d2d_send, d2d_recv, meta_send, meta_recv, ret_send, ret_recv, load_sem,
):
    ep = 2 * side * side
    tok, dim = x_ref.shape
    inter = wg.shape[2]
    sinter = hs.shape[1]
    quarter = dim // 4
    lanes = meta.shape[2]
    nexp = router_ref.shape[0]
    me = lax.axis_index("ep")
    core = lax.rem(me, 2)
    chip = lax.div(me, 2)
    my_x = lax.rem(chip, side)
    my_y = lax.div(chip, side)

    peer = me + 1 - 2 * core

    def at(first, second, plane=core, dev_core=None):
        col = lax.rem(my_x + side + second + plane * (first - second), side)
        row = lax.rem(my_y + side + first + plane * (second - first), side)
        return (row * side + col) * 2 + (plane if dev_core is None else dev_core)

    def rows(src, first, count):
        return xall.at[pl.ds(pl.multiple_of((src * 4 + first) * tok, tok), count * tok)]

    barrier = pltpu.get_barrier_semaphore()

    def greet(k, carry):
        pl.semaphore_signal(barrier, inc=1, device_id={"ep": lax.rem(me + k, ep)}, device_id_type=MESH)
        return carry

    lax.fori_loop(1, ep, greet, 0)
    weight_copies = []
    for i, (src, dst) in enumerate(((wg_hbm, wg), (wu_hbm, wu))):
        for e in range(2):
            weight_copies.append(pltpu.make_async_copy(src.at[e], dst.at[e], w_sem.at[i * 2 + e]))
    for e in range(2):
        weight_copies.append(
            pltpu.make_async_copy(wd_hbm.at[pl.ds(e * inter, inter)], wd.at[pl.ds(e * inter, inter)], w_sem.at[4 + e])
        )
    for copy in weight_copies:
        copy.start()

    x = x_ref[...].astype(F32)
    inv = lax.rsqrt(jnp.mean(x * x, axis=1, keepdims=True) + NORM_EPS)
    x_norm = (x * inv * gain_ref[...]).astype(BF16)
    xn[...] = x_norm
    base = pl.multiple_of(me * 4 * tok, tok)
    for q in range(4):
        xall[pl.ds(pl.multiple_of(base + q * tok, tok), tok), :] = x_norm[:, q * quarter : (q + 1) * quarter]

    pl.semaphore_wait(barrier, ep - 1)

    sends = []

    def remote(src, dst, send_sem, recv_sem, target):
        return pltpu.make_async_remote_copy(
            src_ref=src, dst_ref=dst, send_sem=send_sem, recv_sem=recv_sem,
            device_id={"ep": target}, device_id_type=MESH,
        )

    def ag_copy(piece, block, first, count, target):
        view = rows(block, first, count)
        remote(view, view, ag_send.at[piece], ag_recv.at[piece], target).start()
        sends.append((ag_send, piece, count))

    def ag_wait(piece, block, first, count):
        view = rows(block, first, count)
        remote(view, view, ag_send.at[piece], ag_recv.at[piece], at(1, 0)).wait_recv()

    def swap(first, second):
        view = rows(at(first, second), 0, 4)
        slot = (first % side) * side + second % side
        remote(view, view, d2d_send.at[slot], d2d_recv.at[slot], peer).start()
        sends.append((d2d_send, slot, 4))

    def second_axis(line):
        block = at(LINE[line], 0)
        ag_copy(4 + 2 * line, block, 0, 4, at(0, 1))
        ag_copy(5 + 2 * line, block, 0, 4, at(0, -1))

    def first_arrived(way):
        off = (-1, 1)[way]
        block = at(off, 0)
        ag_wait(way, block, 0, 4)
        ag_copy(2 + way, block, 2 * way, 2, at(-off, 0))

    def first_far_arrived():
        block = at(2, 0)
        for way in range(2):
            ag_wait(2 + way, block, 2 * way, 2)
        swap(2, 0)
        second_axis(3)

    def second_arrived(line, way):
        off = (-1, 1)[way]
        block = at(LINE[line], off)
        ag_wait(4 + 2 * line + way, block, 0, 4)
        ag_copy(12 + 2 * line + way, block, 2 * way, 2, at(0, -off))
        swap(LINE[line], off)

    def second_far_arrived(line):
        block = at(LINE[line], 2)
        for way in range(2):
            ag_wait(12 + 2 * line + way, block, 2 * way, 2)
        swap(LINE[line], 2)

    ag_copy(0, me, 0, 4, at(1, 0))
    ag_copy(1, me, 0, 4, at(-1, 0))
    swap(0, 0)

    top = ids_ref.shape[1]
    unit = lax.broadcasted_iota(jnp.int32, (8, top), 0) == lax.broadcasted_iota(jnp.int32, (8, top), 1)
    ids = dot(jnp.where(unit, 1.0, 0.0).astype(BF16), ids_ref[...].astype(F32).astype(BF16), NT)
    ids = jnp.concatenate([ids, jnp.full((8, lanes - tok), -1.0, F32)], axis=1)
    expert = lax.broadcasted_iota(jnp.int32, (nexp, lanes), 0).astype(F32)
    hot = expert == ids[0:1, :]
    for k in range(1, top):
        hot = jnp.logical_or(hot, expert == ids[k : k + 1, :])
    hot = jnp.where(hot, 1.0, 0.0)
    hot_b = hot.astype(BF16)
    upper = lax.broadcasted_iota(jnp.int32, (lanes, lanes), 0) < lax.broadcasted_iota(jnp.int32, (lanes, lanes), 1)
    before = dot(hot_b, jnp.where(upper, 1.0, 0.0).astype(BF16))
    e_row = lax.broadcasted_iota(jnp.int32, (nexp, nexp), 0)
    e_col = lax.broadcasted_iota(jnp.int32, (nexp, nexp), 1)
    same_dev = jnp.where(lax.shift_right_logical(e_row, 1) == lax.shift_right_logical(e_col, 1), 1.0, 0.0).astype(BF16)
    is_odd = jnp.bitwise_and(e_row, 1) == 1
    prev = jnp.where(jnp.logical_and(is_odd, e_col == e_row - 1), 1.0, 0.0).astype(BF16)
    rank = dot(same_dev, before.astype(BF16)) + dot(prev, hot_b)
    rank = jnp.where(hot > 0.5, rank, -1.0)
    r_hi, r_mid, r_lo = split3(router_ref[...])
    logits = dot(r_hi, x_norm, NT) + dot(r_mid, x_norm, NT) + dot(r_lo, x_norm, NT)
    picked = jnp.where(hot[:, :tok] > 0.5, jax.nn.sigmoid(logits), 0.0)
    gates = ROUTE_SCALE * picked / jnp.sum(picked, axis=0, keepdims=True)
    for d in range(ep):
        meta[d, 0:2, :] = rank[2 * d : 2 * d + 2, :]
        meta[d, 2:4, 0:tok] = gates[2 * d : 2 * d + 2, :]

    def meta_copy(k):
        target = lax.rem(me + k, ep)
        return remote(meta.at[target], meta_in.at[me], meta_send.at[k], meta_recv.at[me], target)

    def send_meta(k, carry):
        meta_copy(k).start()
        return carry

    first_arrived(0)
    first_arrived(1)
    lax.fori_loop(1, ep, send_meta, 0)
    own_meta = pltpu.make_async_copy(meta.at[me], meta_in.at[me], meta_recv.at[me])
    own_meta.start()
    second_axis(0)
    for way in range(2):
        swap((-1, 1)[way], 0)
        second_axis(1 + way)
    first_far_arrived()

    gate_events = (
        ((), ((second_arrived, 0, 0), (second_arrived, 0, 1)), (), (), ((second_arrived, 1, 0), (second_arrived, 1, 1))),
        ((), ((second_arrived, 2, 0), (second_arrived, 2, 1)), (), (), ()),
        ((), ((second_far_arrived, 0),), (), (), ((second_far_arrived, 1),)),
    )
    down_events = (
        (),
        ((), ((second_arrived, 3, 0), (second_arrived, 3, 1))),
        ((), ((second_far_arrived, 2),), (), (), (), ((second_far_arrived, 3),)),
    )

    tile = 256
    per = 2 * len(CHUNKS[0])
    full, left = inter // tile, inter % tile
    down_tiles = dim // tile

    def source(c, j):
        first, second = CHUNKS[c][j % (per // 2)]
        return at(first, second, core if j < per // 2 else 1 - core)

    def wait_meta(src):
        remote(meta.at[0], meta_in.at[src], meta_send.at[1], meta_recv.at[src], src).wait_recv()

    def select(c):
        slot_no = lax.broadcasted_iota(jnp.int32, (cap, tok), 0).astype(F32)
        for j in range(per):
            src = source(c, j)
            if c == 0 and j == 0:
                own_meta.wait()
            else:
                wait_meta(src)
            if j >= per // 2:
                first, second = CHUNKS[c][j % (per // 2)]
                slot = (first % side) * side + second % side
                view = rows(src, 0, 4)
                remote(view, view, d2d_send.at[slot], d2d_recv.at[slot], peer).wait_recv()
            low = jnp.where(slot_no == meta_in[src, 0:1, 0:tok], 1.0, 0.0)
            high = jnp.where(slot_no == meta_in[src, 1:2, 0:tok], 1.0, 0.0)
            mask[j * cap : (j + 1) * cap, :] = jnp.broadcast_to(jnp.sum(low, axis=1, keepdims=True), (cap, tile))
            pick = (low + high).astype(BF16)
            for q in range(4):
                block = xall[pl.ds(pl.multiple_of((src * 4 + q) * tok, tok), tok), :]
                xs[j * cap : (j + 1) * cap, q * quarter : (q + 1) * quarter] = dot(pick, block).astype(BF16)

    def gated(gate, up, is_low, keep_low):
        keep = is_low > 0.5
        keep = keep if keep_low else jnp.logical_not(keep)
        return jnp.where(keep, jax.nn.silu(gate) * up, 0.0).astype(BF16)

    def gate_up(n, carry):
        cols = pl.ds(pl.multiple_of(n * tile, tile), tile)
        for e in range(2):
            gate = dot(xs[...], wg[e, :, cols])
            up = dot(xs[...], wu[e, :, cols])
            h[:, pl.ds(pl.multiple_of(e * inter + n * tile, 128), tile)] = gated(gate, up, mask[...], e == 0)
        return carry

    def gate_up_left():
        cols = slice(full * tile, inter)
        for e in range(2):
            both = dot(xs[...], jnp.concatenate([wg[e, :, cols], wu[e, :, cols]], axis=1))
            h[:, e * inter + full * tile : (e + 1) * inter] = gated(both[:, :left], both[:, left:], mask[:, :left], e == 0)

    def down(c, n):
        cols = pl.ds(pl.multiple_of(n * tile, tile), tile)
        y = dot(h[...], wd[:, cols]).astype(BF16)
        outb[c * per : (c + 1) * per, :, cols] = y.reshape(per, cap, tile)

    def run_events(n, table):
        for k, calls in enumerate(table):
            if calls:

                @pl.when(n == k)
                def _():
                    for fn, *args in calls:
                        fn(*args)

    ret_copies = []

    def send_back(c):
        for j in range(per):
            block = outb.at[c * per + j]
            if c == 0 and j == 0:
                copy = pltpu.make_async_copy(block, recv_hbm.at[me], ret_recv.at[me])
            else:
                copy = remote(block, recv_hbm.at[me], ret_send.at[c * per + j], ret_recv.at[me], source(c, j))
            copy.start()
            ret_copies.append(copy)

    for c in range(len(CHUNKS)):
        select(c)
        if c > 0:
            send_back(c - 1)
        if c == 0:
            for copy in weight_copies[:4]:
                copy.wait()

        def gate_step(n, carry, c=c):
            gate_up(n, 0)
            if c < len(gate_events):
                run_events(n, gate_events[c])
            return carry

        lax.fori_loop(0, full, gate_step, 0)
        if left:
            gate_up_left()
        if c == 0:
            for copy in weight_copies[4:]:
                copy.wait()

        def down_step(n, carry, c=c):
            down(c, n)
            if c < len(down_events):
                run_events(n, down_events[c])
            return carry

        lax.fori_loop(0, down_tiles, down_step, 0)

    for sems, i, count in sends:
        view = rows(me, 0, count)
        remote(view, view, sems.at[i], ag_recv.at[0], peer).wait_send()
    s_tile = quarter
    s_steps = [(n * s_tile, min(s_tile, sinter - n * s_tile)) for n in range(-(-sinter // s_tile))]
    pair_slots = xall.shape[0] // (2 * dim)
    pairs = []
    for n, (col, width) in enumerate(s_steps):
        top_row = (n % pair_slots) * 2 * dim
        views = [xall.at[pl.ds(top_row + i * dim, dim), pl.ds(0, width)] for i in range(2)]
        pairs.append([
            pltpu.make_async_copy(w.at[:, pl.ds(col, width)], views[i], s_sem.at[2 * (n % pair_slots) + i])
            for i, w in enumerate((sg_hbm, su_hbm))
        ])
    downs = [
        pltpu.make_async_copy(
            sd_hbm.at[:, pl.ds(n * s_tile, s_tile)], xall.at[pl.ds(n * sinter, sinter), :], s_sem.at[2 * pair_slots + n]
        )
        for n in range(4)
    ]
    for n in range(min(pair_slots, len(pairs))):
        for copy in pairs[n]:
            copy.start()
    send_back(len(CHUNKS) - 1)

    started = 0
    for n, (col, width) in enumerate(s_steps):
        for copy in pairs[n]:
            copy.wait()
        top_row = (n % pair_slots) * 2 * dim
        gate = dot(xn[...], xall[top_row : top_row + dim, 0:width])
        up = dot(xn[...], xall[top_row + dim : top_row + 2 * dim, 0:width])
        hs[:, col : col + width] = (jax.nn.silu(gate) * up).astype(BF16)
        if n + pair_slots < len(pairs):
            for copy in pairs[n + pair_slots]:
                copy.start()
        busy = [(m % pair_slots) * 2 * dim for m in range(n + 1, min(n + 1 + pair_slots, len(pairs)))]
        while started < 4 and all(
            (started + 1) * sinter <= b or started * sinter >= b + 2 * dim for b in busy
        ):
            if n + pair_slots < len(pairs):
                break
            downs[started].start()
            started += 1
    for n in range(4):
        downs[n].wait()
        cols = slice(n * s_tile, (n + 1) * s_tile)
        y = dot(hs[...], xall[n * sinter : (n + 1) * sinter, :]).astype(BF16)
        acc[:, cols] = x_ref[:, cols].astype(F32) + y.astype(F32)

    slot_no = lax.broadcasted_iota(jnp.int32, (cap, lanes), 0).astype(F32)
    valid = lax.broadcasted_iota(jnp.int32, (1, lanes), 1) < tok
    for c in range(len(CHUNKS)):
        loads = []
        weights = []

        def worker(j, c=c):
            first, second = CHUNKS[c][j % (per // 2)]
            return at(-first, -second, core, core if j < per // 2 else 1 - core)

        for j in range(per):
            dev = worker(j)
            low = jnp.where(slot_no == meta[dev, 0:1, :], jnp.where(valid, meta[dev, 2:3, :], 0.0), 0.0)
            high = jnp.where(slot_no == meta[dev, 1:2, :], jnp.where(valid, meta[dev, 3:4, :], 0.0), 0.0)
            weights.append(low + high)
        w_all = jnp.concatenate(weights, axis=0).T
        for i, part in enumerate(split3(w_all)):
            mix[i * tok : (i + 1) * tok, :] = part[:tok]
        for j in range(per):
            dev = worker(j)
            if c == 0 and j == 0:
                ret_copies[0].wait()
            else:
                remote(outb.at[0], recv_hbm.at[dev], ret_send.at[1], ret_recv.at[dev], dev).wait_recv()
            load = pltpu.make_async_copy(recv_hbm.at[dev], xs.at[pl.ds(j * cap, cap)], load_sem.at[j])
            load.start()
            loads.append(load)
        for load in loads:
            load.wait()
        for q in range(4):
            cols = slice(q * quarter, (q + 1) * quarter)
            block = xs[:, cols]
            part = dot(mix[...], block)
            total = acc[:, cols] + (part[:tok] + part[tok : 2 * tok] + part[2 * tok :])
            if c == len(CHUNKS) - 1:
                out_ref[:, cols] = total.astype(BF16)
            else:
                acc[:, cols] = total

    def meta_sent(k, carry):
        meta_copy(k).wait_send()
        return carry

    lax.fori_loop(1, ep, meta_sent, 0)
    for copy in ret_copies[1:]:
        copy.wait_send()


def solution(mesh):
    ep_size = mesh.shape["ep"]
    side = math.isqrt(ep_size // 2)

    def local_block(hidden_in, norm_gain, router_w, w_gate, w_up, w_down, ws_gate, ws_up, ws_down, expert_ids):
        tok, top_k = expert_ids.shape
        dim = hidden_in.shape[1]
        exp_dev, _, inter = w_gate.shape
        sinter = ws_gate.shape[1]
        cap = GROUPS * ((top_k + GROUP_LIMIT - 1) // GROUP_LIMIT) * tok // ep_size
        lanes = 128
        chunk_rows = cap * 2 * len(CHUNKS[0])
        any_spec = pl.BlockSpec(memory_space=pl.ANY)
        vmem_spec = pl.BlockSpec(memory_space=pltpu.VMEM)
        out, _ = pl.pallas_call(
            functools.partial(moe_kernel, side, cap),
            out_shape=(
                jax.ShapeDtypeStruct((tok, dim), BF16),
                jax.ShapeDtypeStruct((ep_size, cap, dim), BF16),
            ),
            in_specs=[vmem_spec] * 4 + [any_spec] * 6,
            out_specs=(vmem_spec, any_spec),
            scratch_shapes=[
                pltpu.VMEM((exp_dev, dim, inter), BF16),
                pltpu.VMEM((exp_dev, dim, inter), BF16),
                pltpu.VMEM((exp_dev * inter, dim), BF16),
                pltpu.VMEM((ep_size * 4 * tok, dim // 4), BF16),
                pltpu.VMEM((tok, dim), BF16),
                pltpu.VMEM((ep_size, cap, dim), BF16),
                pltpu.VMEM((chunk_rows, dim), BF16),
                pltpu.VMEM((chunk_rows, exp_dev * inter), BF16),
                pltpu.VMEM((chunk_rows, 256), F32),
                pltpu.VMEM((tok, dim), F32),
                pltpu.VMEM((tok, sinter), BF16),
                pltpu.VMEM((3 * tok, chunk_rows), BF16),
                pltpu.VMEM((ep_size, 8, lanes), F32),
                pltpu.VMEM((ep_size, 8, lanes), F32),
                pltpu.SemaphoreType.DMA((6,)),
                pltpu.SemaphoreType.DMA((32,)),
                pltpu.SemaphoreType.DMA((20,)),
                pltpu.SemaphoreType.DMA((20,)),
                pltpu.SemaphoreType.DMA((side * side,)),
                pltpu.SemaphoreType.DMA((side * side,)),
                pltpu.SemaphoreType.DMA((ep_size,)),
                pltpu.SemaphoreType.DMA((ep_size,)),
                pltpu.SemaphoreType.DMA((ep_size,)),
                pltpu.SemaphoreType.DMA((ep_size,)),
                pltpu.SemaphoreType.DMA((8,)),
            ],
            compiler_params=pltpu.CompilerParams(
                collective_id=0, has_side_effects=True, vmem_limit_bytes=67_000_000
            ),
        )(
            hidden_in, norm_gain.reshape(1, dim), router_w, expert_ids, w_gate, w_up,
            w_down.reshape(exp_dev * inter, dim), ws_gate, ws_up, ws_down,
        )
        return out

    row_spec = P(("dp", "ep"), None)
    in_specs = (row_spec, P(), P(), P("ep"), P("ep"), P("ep"), P(), P(), P(), row_spec)
    return jax.shard_map(local_block, mesh=mesh, in_specs=in_specs, out_specs=row_spec, check_vma=False)
```

```python
import functools
import math

import jax
import jax.numpy as jnp
from jax import lax
from jax.experimental import pallas as pl
from jax.experimental.pallas import tpu as pltpu
from jax.sharding import PartitionSpec as P

NORM_EPS = 1e-6
ROUTE_SCALE = 2.5
GROUPS = 8
GROUP_LIMIT = 4
MESH = pl.DeviceIdType.MESH
F32 = jnp.float32
BF16 = jnp.bfloat16
LINE = (0, -1, 1, 2)
CHUNKS = (
    ((0, 0), (1, 0)),
    ((-1, 0), (2, 0)),
    ((-1, -1), (1, 1)),
    ((2, -1), (2, 1)),
    ((1, 2), (-1, 2)),
    ((0, 2), (2, 2)),
    ((1, -1), (-1, 1)),
    ((0, -1), (0, 1)),
)
NT = (((1,), (1,)), ((), ()))


def split3(value):
    hi = value.astype(BF16)
    rest = value - hi.astype(F32)
    mid = rest.astype(BF16)
    lo = (rest - mid.astype(F32)).astype(BF16)
    return hi, mid, lo


def dot(a, b, dims=None):
    dims = (((1,), (0,)), ((), ())) if dims is None else dims
    return lax.dot_general(a, b, dims, preferred_element_type=F32)


def moe_kernel(
    side, cap,
    x_ref, gain_ref, router_ref, ids_ref, wg_hbm, wu_hbm, wd_hbm, sg_hbm, su_hbm, sd_hbm,
    out_ref, recv_hbm,
    wg, wu, wd, xall, xn, outb, xs, h, mask, acc, hs, mix, meta, meta_in,
    w_sem, s_sem, ag_send, ag_recv, d2d_send, d2d_recv, meta_send, meta_recv, ret_send, ret_recv, load_sem,
):
    ep = 2 * side * side
    tok, dim = x_ref.shape
    inter = wg.shape[2]
    sinter = hs.shape[1]
    quarter = dim // 4
    lanes = meta.shape[2]
    nexp = router_ref.shape[0]
    me = lax.axis_index("ep")
    core = lax.rem(me, 2)
    chip = lax.div(me, 2)
    my_x = lax.rem(chip, side)
    my_y = lax.div(chip, side)

    peer = me + 1 - 2 * core

    def at(first, second, plane=core, dev_core=None):
        col = lax.rem(my_x + side + second + plane * (first - second), side)
        row = lax.rem(my_y + side + first + plane * (second - first), side)
        return (row * side + col) * 2 + (plane if dev_core is None else dev_core)

    def rows(src, first, count):
        return xall.at[pl.ds(pl.multiple_of((src * 4 + first) * tok, tok), count * tok)]

    barrier = pltpu.get_barrier_semaphore()

    def greet(k, carry):
        pl.semaphore_signal(barrier, inc=1, device_id={"ep": lax.rem(me + k, ep)}, device_id_type=MESH)
        return carry

    lax.fori_loop(1, ep, greet, 0)
    weight_copies = []
    for i, (src, dst) in enumerate(((wg_hbm, wg), (wu_hbm, wu))):
        for e in range(2):
            weight_copies.append(pltpu.make_async_copy(src.at[e], dst.at[e], w_sem.at[i * 2 + e]))
    for e in range(2):
        weight_copies.append(
            pltpu.make_async_copy(wd_hbm.at[pl.ds(e * inter, inter)], wd.at[pl.ds(e * inter, inter)], w_sem.at[4 + e])
        )
    for copy in weight_copies:
        copy.start()

    x = x_ref[...].astype(F32)
    inv = lax.rsqrt(jnp.mean(x * x, axis=1, keepdims=True) + NORM_EPS)
    x_norm = (x * inv * gain_ref[...]).astype(BF16)
    xn[...] = x_norm
    base = pl.multiple_of(me * 4 * tok, tok)
    for q in range(4):
        xall[pl.ds(pl.multiple_of(base + q * tok, tok), tok), :] = x_norm[:, q * quarter : (q + 1) * quarter]

    pl.semaphore_wait(barrier, ep - 1)

    sends = []

    def remote(src, dst, send_sem, recv_sem, target):
        return pltpu.make_async_remote_copy(
            src_ref=src, dst_ref=dst, send_sem=send_sem, recv_sem=recv_sem,
            device_id={"ep": target}, device_id_type=MESH,
        )

    def ag_copy(piece, block, first, count, target):
        view = rows(block, first, count)
        remote(view, view, ag_send.at[piece], ag_recv.at[piece], target).start()
        sends.append((ag_send, piece, count))

    def ag_wait(piece, block, first, count):
        view = rows(block, first, count)
        remote(view, view, ag_send.at[piece], ag_recv.at[piece], at(1, 0)).wait_recv()

    def swap(first, second):
        view = rows(at(first, second), 0, 4)
        slot = (first % side) * side + second % side
        remote(view, view, d2d_send.at[slot], d2d_recv.at[slot], peer).start()
        sends.append((d2d_send, slot, 4))

    def second_axis(line):
        block = at(LINE[line], 0)
        ag_copy(4 + 2 * line, block, 0, 4, at(0, 1))
        ag_copy(5 + 2 * line, block, 0, 4, at(0, -1))

    def first_arrived(way):
        off = (-1, 1)[way]
        block = at(off, 0)
        ag_wait(way, block, 0, 4)
        ag_copy(2 + way, block, 2 * way, 2, at(-off, 0))

    def first_far_arrived():
        block = at(2, 0)
        for way in range(2):
            ag_wait(2 + way, block, 2 * way, 2)
        swap(2, 0)
        second_axis(3)

    def second_arrived(line, way):
        off = (-1, 1)[way]
        block = at(LINE[line], off)
        ag_wait(4 + 2 * line + way, block, 0, 4)
        ag_copy(12 + 2 * line + way, block, 2 * way, 2, at(0, -off))
        swap(LINE[line], off)

    def second_far_arrived(line):
        block = at(LINE[line], 2)
        for way in range(2):
            ag_wait(12 + 2 * line + way, block, 2 * way, 2)
        swap(LINE[line], 2)

    ag_copy(0, me, 0, 4, at(1, 0))
    ag_copy(1, me, 0, 4, at(-1, 0))
    swap(0, 0)

    top = ids_ref.shape[1]
    unit = lax.broadcasted_iota(jnp.int32, (8, top), 0) == lax.broadcasted_iota(jnp.int32, (8, top), 1)
    ids = dot(jnp.where(unit, 1.0, 0.0).astype(BF16), ids_ref[...].astype(F32).astype(BF16), NT)
    ids = jnp.concatenate([ids, jnp.full((8, lanes - tok), -1.0, F32)], axis=1)
    expert = lax.broadcasted_iota(jnp.int32, (nexp, lanes), 0).astype(F32)
    hot = expert == ids[0:1, :]
    for k in range(1, top):
        hot = jnp.logical_or(hot, expert == ids[k : k + 1, :])
    hot = jnp.where(hot, 1.0, 0.0)
    hot_b = hot.astype(BF16)
    upper = lax.broadcasted_iota(jnp.int32, (lanes, lanes), 0) < lax.broadcasted_iota(jnp.int32, (lanes, lanes), 1)
    before = dot(hot_b, jnp.where(upper, 1.0, 0.0).astype(BF16))
    e_row = lax.broadcasted_iota(jnp.int32, (nexp, nexp), 0)
    e_col = lax.broadcasted_iota(jnp.int32, (nexp, nexp), 1)
    same_dev = jnp.where(lax.shift_right_logical(e_row, 1) == lax.shift_right_logical(e_col, 1), 1.0, 0.0).astype(BF16)
    is_odd = jnp.bitwise_and(e_row, 1) == 1
    prev = jnp.where(jnp.logical_and(is_odd, e_col == e_row - 1), 1.0, 0.0).astype(BF16)
    rank = dot(same_dev, before.astype(BF16)) + dot(prev, hot_b)
    rank = jnp.where(hot > 0.5, rank, -1.0)
    r_hi, r_mid, r_lo = split3(router_ref[...])
    logits = dot(r_hi, x_norm, NT) + dot(r_mid, x_norm, NT) + dot(r_lo, x_norm, NT)
    picked = jnp.where(hot[:, :tok] > 0.5, jax.nn.sigmoid(logits), 0.0)
    gates = ROUTE_SCALE * picked / jnp.sum(picked, axis=0, keepdims=True)
    for d in range(ep):
        meta[d, 0:2, :] = rank[2 * d : 2 * d + 2, :]
        meta[d, 2:4, 0:tok] = gates[2 * d : 2 * d + 2, :]

    def meta_copy(k):
        target = lax.rem(me + k, ep)
        return remote(meta.at[target], meta_in.at[me], meta_send.at[k], meta_recv.at[me], target)

    def send_meta(k, carry):
        meta_copy(k).start()
        return carry

    first_arrived(0)
    first_arrived(1)
    lax.fori_loop(1, ep, send_meta, 0)
    own_meta = pltpu.make_async_copy(meta.at[me], meta_in.at[me], meta_recv.at[me])
    own_meta.start()
    second_axis(0)
    for way in range(2):
        swap((-1, 1)[way], 0)
        second_axis(1 + way)

    gate_events = (
        (((first_far_arrived,),), (), ((second_arrived, 0, 0), (second_arrived, 0, 1)), (), ((second_arrived, 1, 0), (second_arrived, 1, 1))),
        ((), ((second_arrived, 2, 0), (second_arrived, 2, 1)), (), (), ()),
        ((), ((second_far_arrived, 0),), (), (), ((second_far_arrived, 1),)),
    )
    down_events = (
        (),
        ((), ((second_arrived, 3, 0), (second_arrived, 3, 1))),
        ((), ((second_far_arrived, 2),), (), (), (), ((second_far_arrived, 3),)),
    )

    tile = 256
    per = 2 * len(CHUNKS[0])
    full, left = inter // tile, inter % tile
    down_tiles = dim // tile

    def source(c, j):
        first, second = CHUNKS[c][j % (per // 2)]
        return at(first, second, core if j < per // 2 else 1 - core)

    def wait_meta(src):
        remote(meta.at[0], meta_in.at[src], meta_send.at[1], meta_recv.at[src], src).wait_recv()

    def select(c):
        slot_no = lax.broadcasted_iota(jnp.int32, (cap, tok), 0).astype(F32)
        for j in range(per):
            src = source(c, j)
            if c == 0 and j == 0:
                own_meta.wait()
            else:
                wait_meta(src)
            if j >= per // 2:
                first, second = CHUNKS[c][j % (per // 2)]
                slot = (first % side) * side + second % side
                view = rows(src, 0, 4)
                remote(view, view, d2d_send.at[slot], d2d_recv.at[slot], peer).wait_recv()
            low = jnp.where(slot_no == meta_in[src, 0:1, 0:tok], 1.0, 0.0)
            high = jnp.where(slot_no == meta_in[src, 1:2, 0:tok], 1.0, 0.0)
            mask[j * cap : (j + 1) * cap, :] = jnp.broadcast_to(jnp.sum(low, axis=1, keepdims=True), (cap, tile))
            pick = (low + high).astype(BF16)
            for q in range(4):
                block = xall[pl.ds(pl.multiple_of((src * 4 + q) * tok, tok), tok), :]
                xs[j * cap : (j + 1) * cap, q * quarter : (q + 1) * quarter] = dot(pick, block).astype(BF16)

    def gated(gate, up, is_low, keep_low):
        keep = is_low > 0.5
        keep = keep if keep_low else jnp.logical_not(keep)
        return jnp.where(keep, jax.nn.silu(gate) * up, 0.0).astype(BF16)

    def gate_up(n, carry):
        cols = pl.ds(pl.multiple_of(n * tile, tile), tile)
        for e in range(2):
            gate = dot(xs[...], wg[e, :, cols])
            up = dot(xs[...], wu[e, :, cols])
            h[:, pl.ds(pl.multiple_of(e * inter + n * tile, 128), tile)] = gated(gate, up, mask[...], e == 0)
        return carry

    def gate_up_left():
        cols = slice(full * tile, inter)
        for e in range(2):
            both = dot(xs[...], jnp.concatenate([wg[e, :, cols], wu[e, :, cols]], axis=1))
            h[:, e * inter + full * tile : (e + 1) * inter] = gated(both[:, :left], both[:, left:], mask[:, :left], e == 0)

    def down(c, n):
        cols = pl.ds(pl.multiple_of(n * tile, tile), tile)
        y = dot(h[...], wd[:, cols]).astype(BF16)
        outb[c * per : (c + 1) * per, :, cols] = y.reshape(per, cap, tile)

    def run_events(n, table):
        for k, calls in enumerate(table):
            if calls:

                @pl.when(n == k)
                def _():
                    for fn, *args in calls:
                        fn(*args)

    ret_copies = []

    def send_back(c):
        for j in range(per):
            block = outb.at[c * per + j]
            if c == 0 and j == 0:
                copy = pltpu.make_async_copy(block, recv_hbm.at[me], ret_recv.at[me])
            else:
                copy = remote(block, recv_hbm.at[me], ret_send.at[c * per + j], ret_recv.at[me], source(c, j))
            copy.start()
            ret_copies.append(copy)

    for c in range(len(CHUNKS)):
        select(c)
        if c > 0:
            send_back(c - 1)
        if c == 0:
            for copy in weight_copies[:4]:
                copy.wait()

        def gate_step(n, carry, c=c):
            gate_up(n, 0)
            if c < len(gate_events):
                run_events(n, gate_events[c])
            return carry

        lax.fori_loop(0, full, gate_step, 0)
        if left:
            gate_up_left()
        if c == 0:
            for copy in weight_copies[4:]:
                copy.wait()

        def down_step(n, carry, c=c):
            down(c, n)
            if c < len(down_events):
                run_events(n, down_events[c])
            return carry

        lax.fori_loop(0, down_tiles, down_step, 0)

    for sems, i, count in sends:
        view = rows(me, 0, count)
        remote(view, view, sems.at[i], ag_recv.at[0], peer).wait_send()
    s_tile = quarter
    s_steps = [(n * s_tile, min(s_tile, sinter - n * s_tile)) for n in range(-(-sinter // s_tile))]
    pair_slots = xall.shape[0] // (2 * dim)
    pairs = []
    for n, (col, width) in enumerate(s_steps):
        top_row = (n % pair_slots) * 2 * dim
        views = [xall.at[pl.ds(top_row + i * dim, dim), pl.ds(0, width)] for i in range(2)]
        pairs.append([
            pltpu.make_async_copy(w.at[:, pl.ds(col, width)], views[i], s_sem.at[2 * (n % pair_slots) + i])
            for i, w in enumerate((sg_hbm, su_hbm))
        ])
    downs = [
        pltpu.make_async_copy(
            sd_hbm.at[:, pl.ds(n * s_tile, s_tile)], xall.at[pl.ds(n * sinter, sinter), :], s_sem.at[2 * pair_slots + n]
        )
        for n in range(4)
    ]
    for n in range(min(pair_slots, len(pairs))):
        for copy in pairs[n]:
            copy.start()
    send_back(len(CHUNKS) - 1)

    started = 0
    for n, (col, width) in enumerate(s_steps):
        for copy in pairs[n]:
            copy.wait()
        top_row = (n % pair_slots) * 2 * dim
        gate = dot(xn[...], xall[top_row : top_row + dim, 0:width])
        up = dot(xn[...], xall[top_row + dim : top_row + 2 * dim, 0:width])
        hs[:, col : col + width] = (jax.nn.silu(gate) * up).astype(BF16)
        if n + pair_slots < len(pairs):
            for copy in pairs[n + pair_slots]:
                copy.start()
        busy = [(m % pair_slots) * 2 * dim for m in range(n + 1, min(n + 1 + pair_slots, len(pairs)))]
        while started < 4 and all(
            (started + 1) * sinter <= b or started * sinter >= b + 2 * dim for b in busy
        ):
            if n + pair_slots < len(pairs):
                break
            downs[started].start()
            started += 1
    for n in range(4):
        downs[n].wait()
        cols = slice(n * s_tile, (n + 1) * s_tile)
        y = dot(hs[...], xall[n * sinter : (n + 1) * sinter, :]).astype(BF16)
        acc[:, cols] = x_ref[:, cols].astype(F32) + y.astype(F32)

    slot_no = lax.broadcasted_iota(jnp.int32, (cap, lanes), 0).astype(F32)
    valid = lax.broadcasted_iota(jnp.int32, (1, lanes), 1) < tok
    for c in range(len(CHUNKS)):
        loads = []
        weights = []

        def worker(j, c=c):
            first, second = CHUNKS[c][j % (per // 2)]
            return at(-first, -second, core, core if j < per // 2 else 1 - core)

        for j in range(per):
            dev = worker(j)
            low = jnp.where(slot_no == meta[dev, 0:1, :], jnp.where(valid, meta[dev, 2:3, :], 0.0), 0.0)
            high = jnp.where(slot_no == meta[dev, 1:2, :], jnp.where(valid, meta[dev, 3:4, :], 0.0), 0.0)
            weights.append(low + high)
        w_all = jnp.concatenate(weights, axis=0).T
        for i, part in enumerate(split3(w_all)):
            mix[i * tok : (i + 1) * tok, :] = part[:tok]
        for j in range(per):
            dev = worker(j)
            if c == 0 and j == 0:
                ret_copies[0].wait()
            else:
                remote(outb.at[0], recv_hbm.at[dev], ret_send.at[1], ret_recv.at[dev], dev).wait_recv()
            load = pltpu.make_async_copy(recv_hbm.at[dev], xs.at[pl.ds(j * cap, cap)], load_sem.at[j])
            load.start()
            loads.append(load)
        for load in loads:
            load.wait()
        for q in range(4):
            cols = slice(q * quarter, (q + 1) * quarter)
            block = xs[:, cols]
            part = dot(mix[...], block)
            total = acc[:, cols] + (part[:tok] + part[tok : 2 * tok] + part[2 * tok :])
            if c == len(CHUNKS) - 1:
                out_ref[:, cols] = total.astype(BF16)
            else:
                acc[:, cols] = total

    def meta_sent(k, carry):
        meta_copy(k).wait_send()
        return carry

    lax.fori_loop(1, ep, meta_sent, 0)
    for copy in ret_copies[1:]:
        copy.wait_send()


def solution(mesh):
    ep_size = mesh.shape["ep"]
    side = math.isqrt(ep_size // 2)

    def local_block(hidden_in, norm_gain, router_w, w_gate, w_up, w_down, ws_gate, ws_up, ws_down, expert_ids):
        tok, top_k = expert_ids.shape
        dim = hidden_in.shape[1]
        exp_dev, _, inter = w_gate.shape
        sinter = ws_gate.shape[1]
        cap = GROUPS * ((top_k + GROUP_LIMIT - 1) // GROUP_LIMIT) * tok // ep_size
        lanes = 128
        chunk_rows = cap * 2 * len(CHUNKS[0])
        any_spec = pl.BlockSpec(memory_space=pl.ANY)
        vmem_spec = pl.BlockSpec(memory_space=pltpu.VMEM)
        out, _ = pl.pallas_call(
            functools.partial(moe_kernel, side, cap),
            out_shape=(
                jax.ShapeDtypeStruct((tok, dim), BF16),
                jax.ShapeDtypeStruct((ep_size, cap, dim), BF16),
            ),
            in_specs=[vmem_spec] * 4 + [any_spec] * 6,
            out_specs=(vmem_spec, any_spec),
            scratch_shapes=[
                pltpu.VMEM((exp_dev, dim, inter), BF16),
                pltpu.VMEM((exp_dev, dim, inter), BF16),
                pltpu.VMEM((exp_dev * inter, dim), BF16),
                pltpu.VMEM((ep_size * 4 * tok, dim // 4), BF16),
                pltpu.VMEM((tok, dim), BF16),
                pltpu.VMEM((ep_size, cap, dim), BF16),
                pltpu.VMEM((chunk_rows, dim), BF16),
                pltpu.VMEM((chunk_rows, exp_dev * inter), BF16),
                pltpu.VMEM((chunk_rows, 256), F32),
                pltpu.VMEM((tok, dim), F32),
                pltpu.VMEM((tok, sinter), BF16),
                pltpu.VMEM((3 * tok, chunk_rows), BF16),
                pltpu.VMEM((ep_size, 8, lanes), F32),
                pltpu.VMEM((ep_size, 8, lanes), F32),
                pltpu.SemaphoreType.DMA((6,)),
                pltpu.SemaphoreType.DMA((32,)),
                pltpu.SemaphoreType.DMA((20,)),
                pltpu.SemaphoreType.DMA((20,)),
                pltpu.SemaphoreType.DMA((side * side,)),
                pltpu.SemaphoreType.DMA((side * side,)),
                pltpu.SemaphoreType.DMA((ep_size,)),
                pltpu.SemaphoreType.DMA((ep_size,)),
                pltpu.SemaphoreType.DMA((ep_size,)),
                pltpu.SemaphoreType.DMA((ep_size,)),
                pltpu.SemaphoreType.DMA((8,)),
            ],
            compiler_params=pltpu.CompilerParams(
                collective_id=0, has_side_effects=True, vmem_limit_bytes=67_000_000
            ),
        )(
            hidden_in, norm_gain.reshape(1, dim), router_w, expert_ids, w_gate, w_up,
            w_down.reshape(exp_dev * inter, dim), ws_gate, ws_up, ws_down,
        )
        return out

    row_spec = P(("dp", "ep"), None)
    in_specs = (row_spec, P(), P(), P("ep"), P("ep"), P("ep"), P(), P(), P(), row_spec)
    return jax.shard_map(local_block, mesh=mesh, in_specs=in_specs, out_specs=row_spec, check_vma=False)
```
